256 devices in a mesh: path: 128 (over y, z_hi, x, core), shard: 2 (over z_lo).
Axes of the slice: x: 4, y: 4, z: 8 (z_hi: 4, z_lo: 2; z = z_hi * 2 + z_lo), core: 2. Of those that a mesh axis runs over, the one named last changes fastest.
Arguments:
- features: bfloat16 [128, 512, 768], P('path', None, 'shard'), may hold values from -6 to 6
- path_weights: bfloat16 [128, 768, 3072], P('path', None, 'shard'), may hold values from -6 to 6
- cotangent: bfloat16 [128, 512, 3072], P('path', None, 'shard'), may hold values from -6 to 6
- path_module: int32 [128, 1], replicated, may hold values from 0 to 15
- outer_params: float32 [16, 768, 3072], P(None, 'path', 'shard'), may hold values from -6 to 6
- outer_moment: float32 [16, 768, 3072], P(None, 'path', 'shard'), may hold values from -2 to 2
Outputs:
- synced: bfloat16 [128, 768, 3072], P('path', None, 'shard')
- params_new: float32 [16, 768, 3072], P(None, 'path', 'shard')
- moment_new: float32 [16, 768, 3072], P(None, 'path', 'shard')
- grad_weight: bfloat16 [128, 768, 3072], P('path', None, 'shard')
- grad_input: bfloat16 [128, 512, 768], P('path', None, 'shard')
The draws below stay inside these ranges and needn't reach their ends.
Inputs may be any that keep to these rules, and one draw needn't show every extreme that they name: `path_module`: every module id is used by at least one path.
All inputs are finite; a program needn't handle non-finite values.
Results may differ from the reference program's by a relative error of at most 0.005.
Values may be sent and summed in bfloat16 or wider, within the bound.
No kernel may reach another device: no remote copies, remote signals or barrier semaphores. Data moves between devices by JAX's collectives and lax.ppermute only.
A program may use at most 64 MiB of HBM per device.

```python
import jax
import jax.numpy as jnp
from jax import lax

D = 768
FF = 3072
MODULES = 16
TOK = 512
PATHS = 128


def level_of(key, dims, cuts, low, top_value):
    def one(axis_at, blocks):
        heights = jax.random.uniform(jax.random.fold_in(jax.random.fold_in(key, 6), axis_at), (blocks,), jnp.float32, low / len(cuts), top_value / len(cuts))
        return jnp.repeat(jnp.exp(heights), dims[axis_at] // blocks).reshape((-1,) + (1,) * (len(dims) - axis_at - 1))

    gain = one(*cuts[0])
    for cut in cuts[1:]:
        gain = gain * one(*cut)
    return gain


def choose_distinct(own_key, rows, amount, top, lift):
    sequence = jax.random.permutation(jax.random.fold_in(own_key, 1), amount)
    pull = sequence
    for power in range(3):
        pull = pull * pull // amount
    pull = pull * lift // amount
    lots = jax.random.randint(jax.random.fold_in(own_key, 2), (rows, amount), 0, 4096) + pull
    sure = jax.random.permutation(jax.random.fold_in(own_key, 3), rows)[jnp.arange(amount) % rows]
    lots = jnp.where(jnp.arange(rows)[:, None] == sure[None, :], 1 << 14, lots)
    merit = lots * amount + jnp.arange(amount)
    return lax.top_k(merit.astype(jnp.int32), top)[1].astype(jnp.int32)


def gaussian(own_key, extent, deviation, limit, split=(), kind=jnp.bfloat16):
    level = level_of(own_key, extent, split, -0.22, 0.18) if split else 1.0
    array = jax.random.normal(own_key, extent, jnp.float32) * deviation * level
    return jnp.minimum(jnp.maximum(array, -limit), limit).astype(kind)


def setup_inputs(seed: int = 0) -> dict:
    streams_of = jax.random.split(jax.random.key(seed), 7)
    features = gaussian(streams_of[0], (PATHS, TOK, D), 1.0, 6.0, ((0, 128), (2, 2)))
    path_weights = gaussian(streams_of[1], (PATHS, D, FF), 1.0, 6.0, ((0, 128), (2, 2)))
    cotangent = gaussian(streams_of[2], (PATHS, TOK, FF), 1.0, 6.0, ((0, 128), (2, 2)))
    path_module = choose_distinct(streams_of[3], PATHS, MODULES, 1, 512)
    outer_params = gaussian(streams_of[4], (MODULES, D, FF), 1.0, 6.0, ((1, 128), (2, 2)), jnp.float32)
    outer_moment = gaussian(streams_of[5], (MODULES, D, FF), 0.3, 2.0, ((1, 128), (2, 2)), jnp.float32)
    return dict(features=features, path_weights=path_weights, cotangent=cotangent, path_module=path_module, outer_params=outer_params, outer_moment=outer_moment)


outer_momentum = 0.9
outer_rate = 0.7


def silu_slope(pre):
    sigmoid_part = jax.nn.sigmoid(pre)
    return sigmoid_part * (1.0 + pre * (1.0 - sigmoid_part))


def reference(features, path_weights, cotangent, path_module, outer_params, outer_moment):
    multiplier = D ** -0.5

    def inner_layer(operands):
        tokens_in, weights_in, upstream = operands
        pre = jnp.dot(tokens_in, weights_in, preferred_element_type=jnp.float32) * multiplier
        delta = (upstream.astype(jnp.float32) * silu_slope(pre)).astype(jnp.bfloat16)
        grad_w = (jnp.dot(tokens_in.T, delta, preferred_element_type=jnp.float32) * multiplier).astype(jnp.bfloat16)
        grad_in = (jnp.dot(delta, weights_in.T, preferred_element_type=jnp.float32) * multiplier).astype(jnp.bfloat16)
        return grad_w, grad_in

    grad_weight, grad_input = lax.map(inner_layer, (features, path_weights, cotangent))
    modules = path_module[:, 0].astype(jnp.int32)

    def add_path(totals, operands):
        module_id, weights_in = operands
        return totals.at[module_id].add(weights_in.astype(jnp.float32)), None

    totals, unused = lax.scan(add_path, jnp.zeros((MODULES, D, FF), jnp.float32), (modules, path_weights))
    member = (modules[None, :] == jnp.arange(MODULES, dtype=jnp.int32)[:, None]).astype(jnp.float32)
    counts = jnp.sum(member, axis=1)
    average = totals / counts[:, None, None]
    pseudo = outer_params - average
    moment_new = outer_momentum * outer_moment + pseudo
    params_new = outer_params - outer_rate * (pseudo + outer_momentum * moment_new)
    rounded = params_new.astype(jnp.bfloat16)
    synced = rounded[modules]
    return synced, params_new, moment_new, grad_weight, grad_input
```

```python
import functools

import jax
import jax.numpy as jnp
from jax import lax
from jax.experimental import pallas as pl
from jax.experimental.pallas import tpu as pltpu
from jax.sharding import Mesh, PartitionSpec as P

D = 768
FF_HERE = 1536
MODULES = 16
COLS_A = 1024
COLS_B = FF_HERE - COLS_A
BLOCK = 256
PLANE = ("y", "x", "core")
PATH = ("y", "zh", "x", "core")

outer_momentum = 0.9
outer_rate = 0.7

bf16 = jnp.bfloat16
f32 = jnp.float32
i32 = jnp.int32


def silu_slope(pre):
    sigmoid_part = jax.nn.sigmoid(pre)
    return sigmoid_part * (1.0 + pre * (1.0 - sigmoid_part))


def mm(a, b):
    return jnp.dot(a, b, preferred_element_type=f32)


def mm_nt(a, b):
    return lax.dot_general(a, b, (((1,), (1,)), ((), ())), preferred_element_type=f32)


def iota(shape, axis):
    return lax.broadcasted_iota(i32, shape, axis)


def sixth(i):
    return (i * 10923) >> 16


def hot(mask):
    return jnp.where(mask, 1.0, 0.0).astype(bf16)


def message_parts(i):
    v = sixth(i)
    return v >> 2, v & 3, i - 6 * v


def natural_row(peer, zh, r):
    return (((((peer >> 3) * 4) + zh) << 3) + (peer & 7)) * 6 + r


def path_of(peer, zh):
    return ((((peer >> 3) * 4) + zh) << 3) + (peer & 7)


def call(kernel, ins, in_specs, out_shapes, out_specs, grid, zh, scratch=(), flops=0, aliases=None):
    return pl.pallas_call(
        kernel,
        grid_spec=pltpu.PrefetchScalarGridSpec(
            num_scalar_prefetch=1,
            grid=grid,
            in_specs=in_specs,
            out_specs=out_specs,
            scratch_shapes=list(scratch),
        ),
        out_shape=out_shapes,
        input_output_aliases=aliases or {},
        cost_estimate=pl.CostEstimate(flops=flops, bytes_accessed=4 << 20, transcendentals=0),
        compiler_params=pltpu.CompilerParams(vmem_limit_bytes=40 << 20),
    )(zh, *ins)


def cols(rows, first=0):
    return pl.BlockSpec((rows, BLOCK), lambda j, z: (0, j + first))


def whole(rows, width):
    return pl.BlockSpec((rows, width), lambda j, z: (0, 0))


def shape(rows, width, kind):
    return jax.ShapeDtypeStruct((rows, width), kind)


FLOPS = 2 * 768 * 768


def strips_kernel(z, *refs):
    for k in range(4):
        refs[4 + k][...] = refs[k][...].reshape(192, COLS_B)


def strips(weights, zh):
    view = weights.reshape(4, 4, 48, FF_HERE)
    specs = [
        pl.BlockSpec((4, 1, 48, COLS_B), functools.partial(lambda j, z, d: (0, (z[0] + d) & 3, 0, COLS_A // COLS_B), d=d))
        for d in range(4)
    ]
    return call(
        strips_kernel, [view] * 4, specs, [shape(192, COLS_B, bf16)] * 4, [whole(192, COLS_B)] * 4, (1,), zh, flops=FLOPS * 256
    )


def pack_a_kernel(z, w, out, perm):
    @pl.when(pl.program_id(0) == 0)
    def _():
        i = iota((1, 768), 1)
        u = sixth(i)
        peer = ((u >> 5) << 3) + (u & 7)
        target = peer * 24 + ((u >> 3) & 3) * 6 + i - 6 * u
        perm[...] = hot(iota((768, 768), 0) == target)

    out[...] = mm(perm[...], w[...]).astype(bf16)


def pack_a(weights, zh):
    return call(
        pack_a_kernel, [weights], [cols(768)], shape(768, COLS_A, bf16), cols(768), (COLS_A // BLOCK,), zh,
        [pltpu.VMEM((768, 768), bf16)], FLOPS * COLS_A,
    )


def pack_b_kernel(z, b0, b1, b2, b3, out, perm):
    @pl.when(pl.program_id(0) == 0)
    def _():
        k = iota((1, 768), 1)
        v = sixth(k)
        target = (v & 31) * 24 + (v >> 5) * 6 + k - 6 * v
        perm[...] = hot(iota((768, 768), 0) == target)

    out[...] = mm(perm[...], jnp.concatenate([b0[...], b1[...], b2[...], b3[...]], axis=0)).astype(bf16)


def pack_b(blocks, zh):
    return call(
        pack_b_kernel, blocks, [cols(192)] * 4, shape(768, COLS_B, bf16), cols(768), (COLS_B // BLOCK,), zh,
        [pltpu.VMEM((768, 768), bf16)], FLOPS * COLS_B,
    )


def module_rows(mods, rows):
    return hot((iota((rows, 128), 0) & 15) == mods[...])


def sum_a_kernel(z, mods, msg, o0, o1, o2, o3, pick):
    zh = z[0]

    @pl.when(pl.program_id(0) == 0)
    def _():
        peer, q, r = message_parts(iota((1, 768), 1))
        lanes = mm(module_rows(mods, 96), hot(iota((128, 768), 0) == path_of(peer, zh)))
        lanes = jnp.where((iota((96, 768), 0) >> 4) == r, lanes, 0.0)
        for d in range(4):
            pick[d * 96 : (d + 1) * 96, :] = jnp.where(q == ((zh + d) & 3), lanes, 0.0).astype(bf16)

    sums = mm(pick[...], msg[...])
    o0[...] = sums[0:96]
    o1[...] = sums[96:192].astype(bf16)
    o2[...] = sums[192:288].astype(bf16)
    o3[...] = sums[288:384].astype(bf16)


def sum_a(mods, msg, zh):
    return call(
        sum_a_kernel, [mods, msg], [whole(1, 128), cols(768)],
        [shape(96, COLS_A, f32)] + [shape(96, COLS_A, bf16)] * 3, [cols(96)] * 4, (COLS_A // BLOCK,), zh,
        [pltpu.VMEM((384, 768), bf16)], FLOPS * COLS_A // 2,
    )


def outer_step(summed, counts, params, moment):
    pseudo = params - summed / counts
    moment_new = outer_momentum * moment + pseudo
    params_new = params - outer_rate * (pseudo + outer_momentum * moment_new)
    return params_new, moment_new


def count_rows(mods):
    return jnp.sum(module_rows(mods, 96).astype(f32), axis=1, keepdims=True)


def step_a_kernel(z, mods, s0, s1, s2, s3, params, moment, new_params, new_moment, rounded):
    summed = s0[...] + s1[...].astype(f32) + s2[...].astype(f32) + s3[...].astype(f32)
    p, m = outer_step(summed, count_rows(mods), params[...], moment[...])
    new_params[...] = p
    new_moment[...] = m
    rounded[...] = p.astype(bf16)


def step_a(mods, sums, params, moment, zh):
    return call(
        step_a_kernel, [mods, *sums, params, moment], [whole(1, 128)] + [cols(96)] * 6,
        [shape(96, COLS_A, f32)] * 2 + [shape(96, COLS_A, bf16)], [cols(96)] * 3, (COLS_A // BLOCK,), zh, flops=FLOPS * 512,
    )


def step_b_kernel(z, mods, msg, params, moment, new_params, new_moment, out, pick, give):
    zh = z[0]

    @pl.when(pl.program_id(0) == 0)
    def _():
        peer, q, r = message_parts(iota((1, 768), 1))
        lanes = mm(module_rows(mods, 96), hot(iota((128, 768), 0) == path_of(peer, (zh - q) & 3)))
        pick[...] = jnp.where((iota((96, 768), 0) >> 4) == r, lanes, 0.0).astype(bf16)
        peer, q, r = message_parts(iota((768, 128), 0))
        rows = mm_nt(hot(path_of(peer, q) == iota((768, 128), 1)), module_rows(mods, 96))
        r = message_parts(iota((768, 96), 0))[2]
        give[...] = jnp.where(r == (iota((768, 96), 1) >> 4), rows, 0.0).astype(bf16)

    p, m = outer_step(mm(pick[...], msg[...]), count_rows(mods), params[...], moment[...])
    new_params[...] = p
    new_moment[...] = m
    out[...] = mm(give[...], p.astype(bf16)).astype(bf16)


def step_b(mods, msg, params, moment, zh):
    first = COLS_A // BLOCK
    return call(
        step_b_kernel, [mods, msg, params, moment], [whole(1, 128), cols(768), cols(96, first), cols(96, first)],
        [shape(96, COLS_B, f32)] * 2 + [shape(768, COLS_B, bf16)], [cols(96)] * 2 + [cols(768)], (COLS_B // BLOCK,), zh,
        [pltpu.VMEM((96, 768), bf16), pltpu.VMEM((768, 96), bf16)], FLOPS * COLS_B,
    )


def give_a_kernel(z, mods, b0, b1, b2, b3, out, give):
    zh = z[0]

    @pl.when(pl.program_id(0) == 0)
    def _():
        peer = message_parts(iota((768, 128), 0))[0]
        rows = mm_nt(hot(path_of(peer, zh) == iota((768, 128), 1)), module_rows(mods, 384))
        _, q, r = message_parts(iota((768, 384), 0))
        want = q * 6 + r
        give[...] = jnp.where(want == (iota((768, 384), 1) >> 4), rows, 0.0).astype(bf16)

    out[...] = mm(give[...], jnp.concatenate([b0[...], b1[...], b2[...], b3[...]], axis=0)).astype(bf16)


def give_a(mods, blocks, zh):
    return call(
        give_a_kernel, [mods, *blocks], [whole(1, 128)] + [cols(96)] * 4, shape(768, COLS_A, bf16), cols(768),
        (COLS_A // BLOCK,), zh, [pltpu.VMEM((768, 384), bf16)], FLOPS * COLS_A,
    )


def split_b_kernel(z, msg, o0, o1, o2, o3, perm):
    zh = z[0]

    @pl.when(pl.program_id(0) == 0)
    def _():
        peer, q, r = message_parts(iota((1, 768), 1))
        target = ((q - zh) & 3) * 192 + peer * 6 + r
        perm[...] = hot(iota((768, 768), 0) == target)

    rows = mm(perm[...], msg[...]).astype(bf16)
    for d, ref in enumerate((o0, o1, o2, o3)):
        ref[...] = rows[d * 192 : (d + 1) * 192]


def split_b(msg, zh):
    return call(
        split_b_kernel, [msg], [cols(768)], [shape(192, COLS_B, bf16)] * 4, [cols(192)] * 4, (COLS_B // BLOCK,), zh,
        [pltpu.VMEM((768, 768), bf16)], FLOPS * COLS_B,
    )


def out_spec(first):
    return pl.BlockSpec((4, 4, 48, BLOCK), lambda j, z: (0, 0, 0, j + first))


OUT = jax.ShapeDtypeStruct((4, 4, 48, FF_HERE), bf16)


def final_a_kernel(z, msg, out, perm):
    zh = z[0]

    @pl.when(pl.program_id(0) == 0)
    def _():
        peer, q, r = message_parts(iota((1, 768), 1))
        perm[...] = hot(iota((768, 768), 0) == natural_row(peer, (zh - q) & 3, r))

    out[...] = mm(perm[...], msg[...]).astype(bf16).reshape(4, 4, 48, BLOCK)


def final_a(msg, zh):
    return call(
        final_a_kernel, [msg], [cols(768)], OUT, out_spec(0), (COLS_A // BLOCK,), zh,
        [pltpu.VMEM((768, 768), bf16)], FLOPS * COLS_A,
    )


def final_b_kernel(z, b0, b1, b2, b3, old, out):
    for d, ref in enumerate((b0, b1, b2, b3)):
        out[:, pl.ds((z[0] - d) & 3, 1), :, :] = ref[...].reshape(4, 1, 48, BLOCK)


def final_b(blocks, old, zh):
    return call(
        final_b_kernel, [*blocks, old], [cols(192)] * 4 + [pl.BlockSpec(memory_space=pl.ANY)], OUT,
        out_spec(COLS_A // BLOCK), (COLS_B // BLOCK,), zh, flops=FLOPS * 256, aliases={5: 0},
    )


def shift_z(block, d):
    return lax.ppermute(block, "zh", [(i, (i + d) % 4) for i in range(4)])


def shift_all(blocks):
    moved = {d: shift_z(blocks[d], d) for d in (2, 1, 3)}
    return [blocks[0]] + [moved[d] for d in (1, 2, 3)]


def plane_exchange(rows):
    blocks = rows.reshape(32, 24, rows.shape[-1])
    return lax.all_to_all(blocks, PLANE, 0, 0, tiled=True).reshape(rows.shape)


def after(value, earlier):
    return lax.optimization_barrier((value, earlier))


def on_device(features, path_weights, cotangent, path_module, outer_params, outer_moment):
    multiplier = D ** (-0.5)
    weights = path_weights[0]
    zh = lax.axis_index("zh").reshape(1)
    first = lax.axis_index("shard") == 0
    mods = path_module.reshape(1, 128)
    params = outer_params.transpose(1, 0, 2).reshape(96, FF_HERE)
    moment = outer_moment.transpose(1, 0, 2).reshape(96, FF_HERE)

    swap = [(0, 1), (1, 0)]
    other = lax.ppermute(features[0], "shard", swap)

    got_b = shift_all(strips(weights, zh))
    in_a = plane_exchange(pack_a(weights, zh))
    out_b, in_a = after(pack_b(got_b, zh), in_a)
    in_b = plane_exchange(out_b)

    sums_a = shift_all(sum_a(mods, in_a, zh))
    params_a, moment_a, mine_a = step_a(mods, sums_a, params, moment, zh)
    params_b, moment_b, back_out_b = step_b(mods, in_b, params, moment, zh)
    back_b = plane_exchange(back_out_b)

    every_a = shift_all([mine_a] * 4)
    back_out_a, back_b = after(give_a(mods, every_a, zh), back_b)
    back_a = plane_exchange(back_out_a)

    home_b = shift_all(split_b(back_b, zh))
    synced = final_b(home_b, final_a(back_a, zh), zh).reshape(1, 768, FF_HERE)

    params_new = jnp.concatenate([params_a, params_b], axis=1)
    moment_new = jnp.concatenate([moment_a, moment_b], axis=1)
    params_new = params_new.reshape(6, MODULES, FF_HERE).transpose(1, 0, 2)
    moment_new = moment_new.reshape(6, MODULES, FF_HERE).transpose(1, 0, 2)

    tokens = jnp.concatenate(
        [jnp.where(first, features[0], other), jnp.where(first, other, features[0])], axis=1
    )
    pre = mm(tokens, weights) * multiplier
    delta = (cotangent[0].astype(f32) * silu_slope(pre)).astype(bf16)
    grad_w = lax.dot_general(tokens, delta, (((0,), (0,)), ((), ())), preferred_element_type=f32)
    grad_w = (grad_w * multiplier).astype(bf16)
    terms = mm_nt(delta, weights) * multiplier
    half = D // 2
    give = jnp.where(first, terms[:, half:], terms[:, :half]).astype(bf16)
    keep = jnp.where(first, terms[:, :half], terms[:, half:])
    grad_in = (keep + lax.ppermute(give, "shard", swap).astype(f32)).astype(bf16)
    return (synced, params_new, moment_new, grad_w[None], grad_in[None])


def solution(mesh):
    fine = Mesh(mesh.devices.reshape(4, 4, 4, 2, 2), ("y", "zh", "x", "core", "shard"))
    wide = P(PATH, None, "shard")
    state = P(None, PATH, "shard")
    return jax.shard_map(
        on_device,
        mesh=fine,
        in_specs=(wide, wide, wide, P(), state, state),
        out_specs=(wide, state, state, wide, wide),
        check_vma=False,
    )
```
